32 devices in a mesh: section: 2 (over core), dp: 2 (over y), tensor: 8 (over z, x).
Axes of the slice: x: 2, y: 2, z: 4, core: 2. Of those that a mesh axis runs over, the one named last changes fastest.
Arguments:
- residual_parts: bfloat16 [2, 768, 16384], P('section', 'dp', 'tensor'), may hold values from -120 to 120
- attn_out: bfloat16 [2, 768, 16384], P('section', 'dp', 'tensor'), may hold values from -6 to 6
- ffn_input: bfloat16 [2, 768, 53248], P('section', 'dp', 'tensor'), may hold values from -6 to 6
- norm_gain: float32 [2, 16384], P('section', 'tensor'), may hold values from 0.25 to 1.75
- mixing: bfloat16 [2, 52, 52], P('section'), may hold values from -0.875 to 0.875
- blocks: int32 [2, 2], P('section'), may hold values from 0 to 25, as said below
Outputs:
- hess_in: float32 [2, 16384, 1024], P('section', 'tensor', 'dp')
- hess_o: float32 [2, 16384, 1024], P('section', 'tensor', 'dp')
- hess_down: float32 [2, 2048, 2048], P('section', 'tensor', 'dp')
The draws below stay inside these ranges and needn't reach their ends.
Inputs may be any that keep to these rules, and one draw needn't show every extreme that they name: `blocks`: entry [s, 0] is below 16; entry [s, 1] is below 26. In every draw one layer has entry [s, 0] = 0 and entry [s, 1] = 25.
All inputs are finite; a program needn't handle non-finite values.
Results may differ from the reference program's by a relative error of at most 0.0038.
Values may be sent and summed in bfloat16 or wider, within the bound.
A program may use at most 128 MiB of HBM per device.

```python
import math
import jax
import jax.numpy as jnp
from jax import lax

D = 16384
FF = 53248
KB = 52
HBLK = 1024
BLK = 2048
MB_TOK = 192
KA = 1024
TOKENS = 768
N_SECTION = 2


def draw_residual_parts(key, part):
    key_base, key_rows, key_cols, key_delta = jax.random.split(jax.random.fold_in(key, 11), 4)
    base = jax.random.normal(key_base, (TOKENS, D), jnp.float32)
    row_scale = jnp.exp(jax.random.uniform(key_rows, (TOKENS,), jnp.float32, 0.0, math.log(10.0)))
    rising = jnp.exp(math.log(3.0) * jnp.arange(D, dtype=jnp.float32) / D)
    col_scale = rising * jnp.exp(jax.random.uniform(key_cols, (D,), jnp.float32, 0.0, math.log(10.0))) / 3.0
    stream = base * row_scale[:, None] * col_scale[None, :]
    update = 2.0 * jax.random.normal(key_delta, (TOKENS, D), jnp.float32) * row_scale[:, None]
    parts = jnp.stack([stream, update] + [update] * (N_SECTION - 2))
    return jnp.clip(parts, -120.0, 120.0).astype(jnp.bfloat16)


def draw_blocks(key, part):
    key_in, key_down, key_pick = jax.random.split(jax.random.fold_in(key, 23), 3)
    first = jax.random.randint(key_in, (N_SECTION,), 0, D // HBLK, jnp.int32)
    second = jax.random.randint(key_down, (N_SECTION,), 0, FF // BLK, jnp.int32)
    picked = jax.random.randint(key_pick, (), 0, N_SECTION, jnp.int32)
    is_picked = jnp.arange(N_SECTION, dtype=jnp.int32) == picked
    first = jnp.where(is_picked, 0, first).astype(jnp.int32)
    second = jnp.where(is_picked, FF // BLK - 1, second).astype(jnp.int32)
    return jnp.stack([first, second], axis=1)


def levels(stream_key, dims, pieces, least, high):
    loudness = 1.0
    for dim, blocks in pieces:
        steps = jax.random.uniform(jax.random.fold_in(jax.random.fold_in(stream_key, 6), dim), (blocks,), jnp.float32, least / len(pieces), high / len(pieces))
        loudness = loudness * jnp.repeat(jnp.exp(steps), dims[dim] // blocks).reshape((-1,) + (1,) * (len(dims) - 1 - dim))
    return loudness


def normal_values(stream_key, shape, spread, limit, cuts=(), kind=jnp.bfloat16):
    drawn = spread * jax.random.normal(stream_key, shape, jnp.float32)
    if cuts:
        drawn = drawn * levels(stream_key, shape, cuts, -0.22, 0.18)
    return jnp.clip(drawn, -limit, limit).astype(kind)


def setup_inputs(seed: int = 0) -> dict:
    key_list = jax.random.split(jax.random.key(seed), 7)
    residual_parts = draw_residual_parts(jax.random.fold_in(key_list[6], 71), 0)
    attn_out = normal_values(key_list[1], (N_SECTION, TOKENS, D), 1.0, 6.0, ((0, 2), (1, 2), (2, 8)))
    ffn_input = normal_values(key_list[2], (N_SECTION, TOKENS, FF), 1.0, 6.0, ((0, 2), (1, 2), (2, 8)))
    norm_gain = jnp.clip(1.0 + 0.15 * jax.random.normal(key_list[3], (N_SECTION, D), jnp.float32), 0.25, 1.75)
    mixing = normal_values(key_list[4], (N_SECTION, KB, KB), KB ** -0.5, 0.875, ((0, 2),))
    blocks = draw_blocks(jax.random.fold_in(key_list[6], 71), 0)
    return {"residual_parts": residual_parts, "attn_out": attn_out, "ffn_input": ffn_input, "norm_gain": norm_gain, "mixing": mixing, "blocks": blocks}


EPS = 1e-05

def bit_parity(values):
    total = jnp.zeros_like(values)
    for position in range(16):
        total = total + values // (1 << position) % 2
    return total % 2

def sylvester(order):
    index = jnp.arange(order, dtype=jnp.int32)
    parity = bit_parity(jnp.bitwise_and(index[:, None], index[None, :]))
    return (1 - 2 * parity).astype(jnp.float32)

def gram(left, right):
    return jnp.dot(left.T, right, preferred_element_type=jnp.float32)

def down_block(hidden, mixing_one, start):
    width_a = BLK // KB + 2
    first_a = jnp.minimum(start // KB, KA - width_a).astype(jnp.int32)
    chosen = lax.dynamic_slice_in_dim(sylvester(KA), first_a, width_a, 1)
    inner = (start - first_a * KB).astype(jnp.int32)
    factor = mixing_one.astype(jnp.float32)

    def one_block(token_rows):
        cube = token_rows.astype(jnp.float32).reshape(MB_TOK, KA, KB)
        mixed = jnp.einsum('rak,kc->rac', cube, factor, precision=lax.Precision.HIGHEST)
        turned = jnp.einsum('rac,ae->rec', mixed, chosen, precision=lax.Precision.HIGHEST)
        turned = turned / math.sqrt(KA)
        flat = turned.reshape(MB_TOK, width_a * KB)
        return lax.dynamic_slice_in_dim(flat, inner, BLK, 1).astype(jnp.bfloat16)
    grouped = hidden.reshape(TOKENS // MB_TOK, MB_TOK, FF)
    return lax.map(one_block, grouped).reshape(TOKENS, BLK)

def reference(residual_parts, attn_out, ffn_input, norm_gain, mixing, blocks):
    scale = 2.0 / TOKENS
    list_in, list_o, list_down = ([], [], [])
    for layer in range(N_SECTION):
        layer_in = residual_parts[layer].astype(jnp.float32)
        if layer > 0:
            layer_in = residual_parts[layer - 1].astype(jnp.float32) + layer_in
        mean_sq = lax.optimization_barrier(jnp.mean(layer_in * layer_in, axis=1))
        normed = (layer_in * lax.rsqrt(mean_sq + EPS)[:, None] * norm_gain[layer][None, :]).astype(jnp.bfloat16)
        first = (blocks[layer, 0] * HBLK).astype(jnp.int32)
        norm_cols = lax.dynamic_slice_in_dim(normed, first, HBLK, 1)
        list_in.append(scale * gram(normed, norm_cols))
        attention = attn_out[layer]
        attn_cols = lax.dynamic_slice_in_dim(attention, first, HBLK, 1)
        list_o.append(scale * gram(attention, attn_cols))
        start = (blocks[layer, 1] * BLK).astype(jnp.int32)
        down_cols = down_block(ffn_input[layer], mixing[layer], start)
        list_down.append(scale * gram(down_cols, down_cols))
    return (jnp.stack(list_in), jnp.stack(list_o), jnp.stack(list_down))
```

```python
import functools
import math

import jax
import jax.numpy as jnp
from jax import lax
from jax.experimental import pallas as pl
from jax.experimental.pallas import tpu as pltpu
from jax.sharding import PartitionSpec as P

D = 16384
KB = 52
HBLK = 1024
BLK = 2048
GROUP = 32


EPS = 1e-05

MESH = pl.DeviceIdType.MESH


def passed_along(x, axis, by):
    devices = lax.axis_size(axis)
    pairs = [(i, i + by) for i in range(devices) if 0 <= i + by < devices]
    return lax.ppermute(x, axis, pairs)


def shifted(x, axis, by):
    devices = lax.axis_size(axis)
    return lax.ppermute(x, axis, [(i, (i + by) % devices) for i in range(devices)])


def gathered(x, axis):
    return [x] + [shifted(x, axis, by) for by in range(1, lax.axis_size(axis))]


def reduce_kernel(n, extras, *refs):
    x_ref, refs = refs[0], refs[1:]
    e_ref, refs = (refs[0], refs[1:]) if extras else (None, refs)
    out_ref, refs = refs[0], refs[1:]
    eout_ref, refs = (refs[0], refs[1:]) if extras else (None, refs)
    recv, mine, send_a, recv_a, send_b, recv_b = refs[:6]
    me = lax.axis_index("tensor")

    barrier = pltpu.get_barrier_semaphore()
    for k in range(1, n):
        pl.semaphore_signal(
            barrier, inc=1, device_id={"tensor": lax.rem(me + k, n)}, device_id_type=MESH
        )
    pl.semaphore_wait(barrier, n - 1)

    def remote(src, dst, send, receive, k):
        return pltpu.make_async_remote_copy(
            src_ref=src,
            dst_ref=dst,
            send_sem=send.at[k],
            recv_sem=receive.at[k],
            device_id={"tensor": lax.rem(me + k, n)},
            device_id_type=MESH,
        )

    order = sorted(range(1, n), key=lambda k: -min(k, n - k))
    extra = []
    if extras:
        erecv, send_e, recv_e = refs[6:]
        extra = [remote(e_ref, erecv.at[k], send_e, recv_e, k) for k in order]
    first = [remote(x_ref.at[lax.rem(me + k, n)], recv.at[k], send_a, recv_a, k) for k in order]
    for copy in extra + first:
        copy.start()
    if extras:
        for copy in extra:
            copy.wait()
        eout_ref[...] = e_ref[...] + functools.reduce(
            lambda a, k: a + erecv[k], range(2, n), erecv[1]
        )
    for copy in first:
        copy.wait()
    total = x_ref[me].astype(jnp.float32)
    for k in range(1, n):
        total = total + recv[k].astype(jnp.float32)
    mine[...] = total.astype(mine.dtype)
    out_ref[me] = total.astype(mine.dtype)
    second = [remote(mine, out_ref.at[me], send_b, recv_b, k) for k in order]
    for copy in second:
        copy.start()
    for copy in second:
        copy.wait()


def tensor_sum(x, extra, ident):
    n = lax.axis_size("tensor")
    rows, columns = x.shape
    x = x.reshape(n, rows // n, columns)
    vmem = pl.BlockSpec(memory_space=pltpu.VMEM)
    operands = [x] + ([extra] if extra is not None else [])
    shapes = [jax.ShapeDtypeStruct(x.shape, jnp.bfloat16)]
    scratch = [
        pltpu.VMEM(x.shape, x.dtype),
        pltpu.VMEM(x.shape[1:], jnp.bfloat16),
    ] + [pltpu.SemaphoreType.DMA((n,))] * 4
    if extra is not None:
        shapes.append(jax.ShapeDtypeStruct(extra.shape, extra.dtype))
        scratch += [pltpu.VMEM((n,) + extra.shape, extra.dtype)]
        scratch += [pltpu.SemaphoreType.DMA((n,))] * 2
    out = pl.pallas_call(
        functools.partial(reduce_kernel, n, extra is not None),
        out_shape=shapes,
        in_specs=[vmem] * len(operands),
        out_specs=[vmem] * len(shapes),
        scratch_shapes=scratch,
        compiler_params=pltpu.CompilerParams(
            collective_id=ident, has_side_effects=True, vmem_limit_bytes=32 << 20
        ),
        cost_estimate=pl.CostEstimate(flops=0, bytes_accessed=100 << 20, transcendentals=0),
    )(*operands)
    return [out[0].reshape(rows, columns)] + list(out[1:])


def parity_sign(values):
    return (1 - 2 * (lax.population_count(values) & 1)).astype(jnp.float32)


def gram(left, right):
    return lax.dot_general(
        left, right, (((0,), (0,)), ((), ())), preferred_element_type=jnp.float32
    )


def local(residual_parts, attn_out, ffn_input, norm_gain, mixing, blocks):
    local_d = residual_parts.shape[2]
    local_f = ffn_input.shape[2]
    token_rows = residual_parts.shape[1]
    dp_count = lax.axis_size("dp")
    dp_member = lax.axis_index("dp")
    tensor_count = lax.axis_size("tensor")
    member = lax.axis_index("tensor")
    own_part = residual_parts[0]
    parts = gathered(own_part, "dp")
    attention = jnp.concatenate(gathered(attn_out[0], "dp"), axis=0)
    earlier = [passed_along(part, "section", 1) for part in parts]
    layers = [
        e.astype(jnp.float32) + p.astype(jnp.float32) for e, p in zip(earlier, parts)
    ]
    squares = jnp.sum(layers[0] * layers[0], axis=1).reshape(token_rows // 128, 128)

    a_local = local_f // KB
    order_a = a_local * tensor_count
    deep = GROUP * KB
    column = blocks[0, 1] * BLK + jnp.arange(BLK, dtype=jnp.int32)
    a_col, c_col = column // KB, column % KB
    pick = (jnp.arange(KB, dtype=jnp.int32)[:, None] == c_col[None, :]).astype(jnp.bfloat16)
    spread = jnp.dot(
        jnp.tile(mixing[0], (GROUP, 1)), pick, preferred_element_type=jnp.float32
    )
    row_a = jnp.arange(deep, dtype=jnp.int32) // KB
    base = (spread * parity_sign(row_a[:, None] & a_col[None, :])).astype(jnp.bfloat16)
    term = None
    for g in range(a_local // GROUP):
        sign = parity_sign((member * a_local + g * GROUP) & a_col) / math.sqrt(order_a)
        piece = jnp.dot(
            ffn_input[0, :, g * deep : (g + 1) * deep], base, preferred_element_type=jnp.float32
        )
        piece = piece * sign[None, :]
        term = piece if term is None else term + piece

    rotated, square_own = tensor_sum(term, squares, 0)

    square_total = gathered(square_own, "dp")
    rotated, square_total = lax.optimization_barrier((rotated, square_total))
    square_total = [s.reshape(token_rows) for s in square_total]
    share = BLK // tensor_count
    own_cols = lax.dynamic_slice_in_dim(rotated, member * share, share, 1)
    part_down = gram(own_cols, rotated)
    half = BLK // dp_count
    if dp_count == 2:
        kept = lax.dynamic_slice_in_dim(part_down, dp_member * half, half, 1)
        sent = lax.dynamic_slice_in_dim(part_down, (1 - dp_member) * half, half, 1)
        sum_down = kept + shifted(sent, "dp", 1)
    else:
        sum_down = lax.psum_scatter(part_down, "dp", scatter_dimension=1, tiled=True)

    normed = jnp.concatenate(
        [
            (x * lax.rsqrt(s / D + EPS)[:, None] * norm_gain[0][None, :]).astype(jnp.bfloat16)
            for x, s in zip(layers, square_total)
        ],
        axis=0,
    )
    first_col = blocks[0, 0] * HBLK
    width = HBLK // dp_count
    offset = first_col % local_d + dp_member * width
    owned = first_col // local_d == member
    slab = jnp.concatenate(
        [
            lax.dynamic_slice_in_dim(normed, offset, width, 1),
            lax.dynamic_slice_in_dim(attention, offset, width, 1),
        ],
        axis=0,
    )
    slab = jnp.where(owned, slab, 0).astype(jnp.bfloat16)
    (got,) = tensor_sum(slab, None, 1)
    tokens = token_rows * dp_count
    scale = 2.0 / tokens
    hess_in = (scale * gram(normed, got[:tokens]))[None]
    hess_o = (scale * gram(attention, got[tokens:]))[None]
    hess_down = (scale * sum_down)[None]
    return (hess_in, hess_o, hess_down)


def solution(mesh):
    return jax.shard_map(
        local,
        mesh=mesh,
        in_specs=(
            P("section", "dp", "tensor"),
            P("section", "dp", "tensor"),
            P("section", "dp", "tensor"),
            P("section", "tensor"),
            P("section", None, None),
            P("section", None),
        ),
        out_specs=(
            P("section", "tensor", "dp"),
            P("section", "tensor", "dp"),
            P("section", "tensor", "dp"),
        ),
        check_vma=False,
    )
```
